1024 devices in a mesh: fsdp: 128 (over y, z_lo, x), seq: 8 (over z_hi, core).
Axes of the slice: x: 4, y: 8, z: 16 (z_hi: 4, z_lo: 4; z = z_hi * 4 + z_lo), core: 2. Of those that a mesh axis runs over, the one named last changes fastest.
Arguments:
- layer_input: bfloat16 [128, 1024, 4096], P('fsdp', 'seq'), may hold values from -24 to 24
- dt_weight: bfloat16 [4096, 64], P('fsdp'), may hold values from -0.09375 to 0.09375
- dt_bias: float32 [64], replicated, may hold values from -2 to -0.5
- decay_rate: float32 [64], replicated, may hold values from 0.0005 to 0.25
- ssm_input: bfloat16 [128, 1024, 2048], P('fsdp', 'seq'), may hold values from -6 to 6
- in_basis: bfloat16 [128, 1024, 512], P('fsdp', 'seq'), may hold values from -0.59765625 to 0.59765625
- out_basis: bfloat16 [128, 1024, 512], P('fsdp', 'seq'), may hold values from -0.59765625 to 0.59765625
- out_cotangent: bfloat16 [128, 1024, 2048], P('fsdp', 'seq'), may hold values from -6 to 6
Outputs:
- grad_input: bfloat16 [128, 1024, 2048], P('fsdp', 'seq')
- grad_in_basis: bfloat16 [128, 1024, 512], P('fsdp', 'seq')
- grad_out_basis: bfloat16 [128, 1024, 512], P('fsdp', 'seq')
- grad_dt_weight: float32 [4096, 64], P('fsdp')
The draws below stay inside these ranges and needn't reach their ends.
All inputs are finite; a program needn't handle non-finite values.
Results may differ from the reference program's by a relative error of at most 0.011.
Values may be sent and summed in bfloat16 or wider, within the bound.
No kernel may reach another device: no remote copies, remote signals or barrier semaphores. Data moves between devices by JAX's collectives and lax.ppermute only.
A program may use at most 64 MiB of HBM per device.

```python
import math
import jax
import jax.numpy as jnp
from jax import lax

D = 4096
HEADS = 64
HEAD_DIM = 32
GROUPS = 4
STATE = 128
TOK_DEV = 128
SEQLEN = 1024
BATCH = 128
N_SEQ = 8


def raised(values, key, source, target, parts, factor):
    owner, partner = [(jnp.arange(values.shape[dim]) // (values.shape[dim] // parts)).reshape([-1 if axis == dim else 1 for axis in range(values.ndim)]) for dim in (source, target)]
    chosen = jax.random.permutation(key, parts)[partner]
    strong = (owner == chosen) | (owner == (partner + parts // 2) % parts)
    return jnp.where(strong, factor * values, values)


def level_of(rng, extent, split, low, largest):
    factor_of = 1.0
    for dim, shards_of in split:
        heights = jax.random.uniform(jax.random.fold_in(jax.random.fold_in(rng, 6), dim), (shards_of,), jnp.float32, low / len(split), largest / len(split))
        factor_of = factor_of * jnp.repeat(jnp.exp(heights), extent[dim] // shards_of).reshape((-1,) + (1,) * (len(extent) - 1 - dim))
    return factor_of


def bell_draw(key, extent, scale, reach, cuts=(), dtype=jnp.bfloat16):
    entries = jax.random.normal(key, extent, jnp.float32) * scale
    if len(cuts) > 0:
        entries = level_of(key, extent, cuts, -0.22, 0.18) * entries
    return jnp.clip(entries, min=-reach, max=reach).astype(dtype)


def gaussian_with(own_key, shape, scale, most, shards, heavy, held_as=jnp.bfloat16):
    array = scale * jax.random.normal(own_key, shape, jnp.float32)
    if shards:
        array = array * level_of(own_key, shape, shards, -0.22, 0.18)
    return jnp.clip(raised(array, jax.random.fold_in(own_key, 3), *heavy), -most, most).astype(held_as)


def setup_inputs(seed: int = 0) -> dict:
    streams_of = jax.random.split(jax.random.key(seed), 9)
    layer_input = gaussian_with(streams_of[0], (BATCH, SEQLEN, D), 1.0, 24.0, ((0, 128), (1, 8)), (0, 2, 128, 5.5))
    dt_weight = bell_draw(streams_of[1], (D, HEADS), D ** -0.5, 0.09375, ((0, 128),))
    dt_bias = jnp.clip(jax.random.uniform(streams_of[2], (HEADS,), jnp.float32, -2.0, -0.5), -2.0, -0.5)
    decay_rate = jnp.clip(jnp.exp(jax.random.uniform(streams_of[3], (HEADS,), jnp.float32, math.log(0.0005), math.log(0.25))), 0.0005, 0.25)
    ssm_input = bell_draw(streams_of[4], (BATCH, SEQLEN, HEADS * HEAD_DIM), 1.0, 6.0, ((0, 128), (1, 8)))
    in_basis = bell_draw(streams_of[5], (BATCH, SEQLEN, GROUPS * STATE), 0.09, 0.59765625, ((0, 128), (1, 8)))
    out_basis = bell_draw(streams_of[6], (BATCH, SEQLEN, GROUPS * STATE), 0.09, 0.59765625, ((0, 128), (1, 8)))
    out_cotangent = bell_draw(streams_of[7], (BATCH, SEQLEN, HEADS * HEAD_DIM), 1.0, 6.0, ((0, 128), (1, 8)))
    return {"layer_input": layer_input, "dt_weight": dt_weight, "dt_bias": dt_bias, "decay_rate": decay_rate, "ssm_input": ssm_input, "in_basis": in_basis, "out_basis": out_basis, "out_cotangent": out_cotangent}


HIGH = lax.Precision.HIGHEST

def block_step(state, pieces):
    logdecay, step_size, inputs, basis_in, basis_out = pieces
    cumulative = jnp.cumsum(logdecay, axis=0)
    final = cumulative[-1]
    rows_first = cumulative.T
    spread = rows_first[:, :, None] - rows_first[:, None, :]
    position = jnp.arange(logdecay.shape[0])
    lower = position[:, None] >= position[None, :]
    decay_mat = jnp.where(lower, jnp.exp(jnp.where(lower, spread, 0.0)), 0.0)
    intersection = jnp.einsum('thn,shn->hts', basis_out, basis_in, precision=HIGH)
    weighted = decay_mat * intersection
    inner = jnp.einsum('hts,sh,shp->thp', weighted, step_size, inputs, precision=HIGH)
    from_state = jnp.exp(cumulative)[:, :, None] * jnp.einsum('hpn,thn->thp', state, basis_out, precision=HIGH)
    tail = jnp.exp(final[None, :] - cumulative) * step_size
    new_state = jnp.exp(final)[:, None, None] * state + jnp.einsum('sh,shp,shn->hpn', tail, inputs, basis_in, precision=HIGH)
    return (new_state, inner + from_state)

def forward(weight, inputs, basis_in, basis_out, tokens, dt_bias, decay_rate):
    raw = jnp.dot(tokens, weight, precision=HIGH) + dt_bias
    step_size = jax.nn.softplus(raw)
    logdecay = -decay_rate * step_size
    per_group = HEADS // GROUPS
    inputs_h = inputs.reshape(N_SEQ, TOK_DEV, HEADS, HEAD_DIM)
    bin_h = jnp.repeat(basis_in.reshape(N_SEQ, TOK_DEV, GROUPS, STATE), per_group, axis=2)
    bout_h = jnp.repeat(basis_out.reshape(N_SEQ, TOK_DEV, GROUPS, STATE), per_group, axis=2)
    start = jnp.zeros((HEADS, HEAD_DIM, STATE), jnp.float32)
    pieces = (logdecay.reshape(N_SEQ, TOK_DEV, HEADS), step_size.reshape(N_SEQ, TOK_DEV, HEADS), inputs_h, bin_h, bout_h)
    _, outputs = lax.scan(block_step, start, pieces)
    return outputs.reshape(N_SEQ * TOK_DEV, HEADS * HEAD_DIM)

def reference(layer_input, dt_weight, dt_bias, decay_rate, ssm_input, in_basis, out_basis, out_cotangent):
    weight = dt_weight.astype(jnp.float32)

    def one_sequence(total, row):
        tokens, inputs, basis_in, basis_out, upstream = row
        tokens = tokens.astype(jnp.float32)

        def local(wmat, xval, bval, cval):
            return forward(wmat, xval, bval, cval, tokens, dt_bias, decay_rate)
        _, pull = jax.vjp(local, weight, inputs.astype(jnp.float32), basis_in.astype(jnp.float32), basis_out.astype(jnp.float32))
        grad_w, grad_x, grad_b, grad_c = pull(upstream.astype(jnp.float32))
        return (total + grad_w, (grad_x.astype(jnp.bfloat16), grad_b.astype(jnp.bfloat16), grad_c.astype(jnp.bfloat16)))
    start = jnp.zeros((D, HEADS), jnp.float32)
    total, (grad_x, grad_b, grad_c) = lax.scan(one_sequence, start, (layer_input, ssm_input, in_basis, out_basis, out_cotangent))
    return (grad_x, grad_b, grad_c, total)
```

```python
import jax
import jax.numpy as jnp
from jax import lax
from jax.sharding import PartitionSpec as P

STATE = 128
CORES = 2

HIGH = lax.Precision.HIGHEST
F32 = jnp.float32
BF16 = jnp.bfloat16


def gathered_rows(rows):
    devices = lax.axis_size("fsdp")
    tiles = jnp.broadcast_to(rows[None], (devices, *rows.shape))
    tiles = lax.all_to_all(tiles, "fsdp", 0, 0, tiled=True)
    return tiles.reshape(devices * rows.shape[0], rows.shape[1])


def summed_rows(partial):
    devices = lax.axis_size("fsdp")
    rows = partial.shape[0] // devices
    tiles = partial.astype(BF16).reshape(devices, rows, partial.shape[1])
    tiles = lax.all_to_all(tiles, "fsdp", 0, 0, tiled=True)
    own = jnp.sum(tiles.astype(F32), axis=0)
    blocks = lax.axis_size("seq")
    copies = jnp.broadcast_to(own[None], (blocks, *own.shape))
    copies = lax.all_to_all(copies, "seq", 0, 0, tiled=True)
    return jnp.sum(copies, axis=0)


def core_swap(value):
    blocks = lax.axis_size("seq")
    return lax.ppermute(value, "seq", [(i, i ^ 1) for i in range(blocks)])


def chip_move(value, moves):
    pairs = [(a * CORES + c, b * CORES + c) for a, b in moves for c in range(CORES)]
    return lax.ppermute(value, "seq", pairs)


def carried_states(forward, backward, decay):
    blocks = lax.axis_size("seq")
    chips = blocks // CORES
    place = lax.axis_index("seq")
    chip, upper = place // CORES, place % CORES == 1
    heads = decay.shape[0]
    half_heads = heads // 2
    rows = forward.shape[0] // 2
    per_head = rows // half_heads
    forward, backward = forward.astype(BF16), backward.astype(BF16)
    high = decay.astype(BF16)
    low = (decay - high.astype(F32)).astype(BF16)
    wide = jnp.broadcast_to(jnp.stack([high, low])[:, :, None], (2, heads, STATE))

    def first(v):
        return lax.slice_in_dim(v, 0, v.shape[-2] // 2, axis=v.ndim - 2)

    def second(v):
        return lax.slice_in_dim(v, v.shape[-2] // 2, v.shape[-2], axis=v.ndim - 2)

    def own(v):
        return jnp.where(upper, second(v), first(v))

    def others(v):
        return jnp.where(upper, first(v), second(v))

    swapped = core_swap(
        jnp.concatenate([others(forward), others(backward), others(wide).reshape(-1, STATE)])
    )
    own_decay = jnp.where(upper, decay[half_heads:], decay[:half_heads])
    got_decay = jnp.sum(
        swapped[2 * rows :].reshape(2, half_heads, STATE)[:, :, 0].astype(F32), axis=0
    )
    got_forward, got_backward = swapped[:rows], swapped[rows : 2 * rows]

    def times(factor, v):
        shaped = v.astype(F32).reshape(half_heads, per_head, STATE) * factor[:, None, None]
        return shaped.reshape(v.shape)

    forward_0 = jnp.where(upper, got_forward, own(forward))
    forward_1 = jnp.where(upper, own(forward), got_forward)
    backward_0 = jnp.where(upper, got_backward, own(backward))
    backward_1 = jnp.where(upper, own(backward), got_backward)
    decay_0 = jnp.where(upper, got_decay, own_decay)
    decay_1 = jnp.where(upper, own_decay, got_decay)
    chip_forward = forward_1.astype(F32) + times(decay_1, forward_0)
    chip_backward = backward_0.astype(F32) + times(decay_0, backward_1)
    chip_decay = decay_0 * decay_1

    entry = jnp.zeros_like(forward_0)
    later = jnp.zeros_like(forward_0)
    for stage in range(chips - 1):
        up, down = (stage, stage + 1), (chips - 1 - stage, chips - 2 - stage)
        going_up = chip == up[0]
        sent = jnp.where(going_up, chip_forward, chip_backward) + times(
            chip_decay, jnp.where(going_up, entry, later)
        )
        got = chip_move(sent.astype(BF16), [up, down])
        entry = jnp.where(chip == up[1], got, entry)
        later = jnp.where(chip == down[1], got, later)

    entry_1 = (forward_0.astype(F32) + times(decay_0, entry)).astype(BF16)
    later_0 = (backward_1.astype(F32) + times(decay_1, later)).astype(BF16)
    mine = jnp.stack([jnp.where(upper, entry_1, entry), jnp.where(upper, later, later_0)])
    theirs = jnp.stack([jnp.where(upper, entry, entry_1), jnp.where(upper, later_0, later)])
    got = core_swap(theirs)
    low_half = jnp.where(upper, got, mine)
    high_half = jnp.where(upper, mine, got)
    both = jnp.concatenate([low_half, high_half], axis=1)
    return both[0], both[1]


def body(
    layer_input, dt_weight, dt_bias, decay_rate, ssm_input, in_basis, out_basis, out_cotangent
):
    tokens = layer_input[0]
    length = tokens.shape[0]
    heads = dt_weight.shape[1]
    groups = in_basis.shape[2] // STATE
    per_group = heads // groups
    head_size = ssm_input.shape[2] // heads
    raw = jnp.dot(tokens, gathered_rows(dt_weight), preferred_element_type=F32) + dt_bias
    step_size = jax.nn.softplus(raw)
    rate_grid = decay_rate.reshape(groups, per_group)
    step_grid = step_size.reshape(length, groups, per_group)
    position = jnp.arange(length)
    lower = position[:, None] >= position[None, :]
    cumulative = jnp.dot(
        lower.astype(F32), -decay_rate * step_size, precision=HIGH
    ).reshape(length, groups, per_group)
    final = cumulative[-1]
    tail = jnp.exp(final[None] - cumulative)
    leading = jnp.exp(cumulative)
    inputs_half = ssm_input[0].reshape(length, groups, per_group, head_size)
    upstream_half = out_cotangent[0].reshape(length, groups, per_group, head_size)
    bin_half = in_basis[0].reshape(length, groups, STATE)
    bout_half = out_basis[0].reshape(length, groups, STATE)
    inputs = inputs_half.astype(F32)
    upstream = upstream_half.astype(F32)
    tailed = ((tail * step_grid)[..., None] * inputs).astype(BF16)
    led = (leading[..., None] * upstream).astype(BF16)
    local_state = jnp.einsum("sgkp,sgn->gkpn", tailed, bin_half, preferred_element_type=F32)
    local_grad = jnp.einsum("tgkp,tgn->gkpn", led, bout_half, preferred_element_type=F32)
    flat = (heads * head_size, STATE)
    entry, later = carried_states(
        local_state.reshape(flat), local_grad.reshape(flat), jnp.exp(final).reshape(heads)
    )
    grid_shape = (groups, per_group, head_size, STATE)
    entry = entry.reshape(grid_shape)
    later = later.reshape(grid_shape)

    cum_rows = cumulative.transpose(1, 2, 0)
    spread = cum_rows[:, :, :, None] - cum_rows[:, :, None, :]
    decay_mat = jnp.where(lower, jnp.exp(jnp.where(lower, spread, 0.0)), 0.0)
    intersection = jnp.einsum("tgn,sgn->gts", bout_half, bin_half, preferred_element_type=F32)
    weighted = (decay_mat * intersection[:, None]).astype(BF16)
    step_cols = step_grid.transpose(1, 2, 0)[:, :, None, :]
    pair = jnp.einsum("tgkp,sgkp->gkts", upstream_half, inputs_half, preferred_element_type=F32)
    through = jnp.einsum("gkts,tgkp->sgkp", weighted, upstream_half, preferred_element_type=F32)
    scaled = decay_mat * pair * step_cols
    joint = jnp.sum(scaled, axis=1).astype(BF16)
    moment = scaled * intersection[:, None]
    change = (jnp.sum(moment, axis=-1) - jnp.sum(moment, axis=-2)).transpose(2, 0, 1)
    local_b = jnp.einsum("gts,tgn->sgn", joint, bout_half, preferred_element_type=F32)
    local_c = jnp.einsum("gts,sgn->tgn", joint, bin_half, preferred_element_type=F32)

    carried = jnp.einsum("sgn,gkpn->sgkp", bin_half, later, preferred_element_type=F32)
    read = jnp.einsum("tgn,gkpn->tgkp", bout_half, entry, preferred_element_type=F32)
    inner_x = through + tail[..., None] * carried
    grad_x = step_grid[..., None] * inner_x
    direct = jnp.sum(inputs * inner_x, axis=-1)
    grad_b = local_b + jnp.einsum("sgkp,gkpn->sgn", tailed, later, preferred_element_type=F32)
    grad_c = local_c + jnp.einsum("tgkp,gkpn->tgn", led, entry, preferred_element_type=F32)
    entry_term = leading * jnp.sum(read * upstream, axis=-1)
    exit_term = tail * step_grid * jnp.sum(inputs * carried, axis=-1)
    closing = jnp.exp(final) * jnp.sum(
        later.astype(F32) * entry.astype(F32), axis=(2, 3)
    ) + jnp.sum(exit_term, axis=0)
    grad_cum = (change + entry_term - exit_term).reshape(length, heads)
    grad_log = jnp.dot((~lower | (position[:, None] == position)).astype(F32), grad_cum, precision=HIGH)
    grad_log = grad_log + closing.reshape(heads)[None]
    grad_step = direct.reshape(length, heads) - decay_rate[None] * grad_log
    grad_raw = grad_step * jax.nn.sigmoid(raw)
    partial = lax.dot_general(
        tokens, grad_raw.astype(BF16), (((0,), (0,)), ((), ())), preferred_element_type=F32
    )
    grad_weight = summed_rows(partial)
    out_x = grad_x.reshape(1, length, heads * head_size).astype(BF16)
    out_b = grad_b.reshape(1, length, groups * STATE).astype(BF16)
    out_c = grad_c.reshape(1, length, groups * STATE).astype(BF16)
    return (out_x, out_b, out_c, grad_weight)


def solution(mesh):
    wide = P("fsdp", "seq", None)
    return jax.shard_map(
        body,
        mesh=mesh,
        in_specs=(wide, P("fsdp", None), P(), P(), wide, wide, wide, wide),
        out_specs=(wide, wide, wide, P("fsdp", None)),
        check_vma=False,
    )
```

```python
import jax
import jax.numpy as jnp
from jax import lax
from jax.sharding import Mesh
from jax.sharding import PartitionSpec as P

STATE = 128
CORES = 2
PARTS = 1
SEQ = ("chip", "core")

HIGH = lax.Precision.HIGHEST
F32 = jnp.float32
BF16 = jnp.bfloat16


def gathered_rows(rows):
    devices = lax.axis_size("fsdp")
    tiles = jnp.broadcast_to(rows[None], (devices, *rows.shape))
    tiles = lax.all_to_all(tiles, "fsdp", 0, 0, tiled=True)
    return tiles.reshape(devices * rows.shape[0], rows.shape[1])


def summed_rows(partial):
    devices = lax.axis_size("fsdp")
    rows = partial.shape[0] // devices
    tiles = partial.astype(BF16).reshape(devices, rows, partial.shape[1])
    tiles = lax.all_to_all(tiles, "fsdp", 0, 0, tiled=True)
    own = jnp.sum(tiles.astype(F32), axis=0)
    blocks = lax.axis_size(SEQ)
    copies = jnp.broadcast_to(own[None], (blocks, *own.shape))
    copies = lax.all_to_all(copies, SEQ, 0, 0, tiled=True)
    return jnp.sum(copies, axis=0)


def core_swap(value):
    return lax.ppermute(value, "core", [(0, 1), (1, 0)])


def halves(value, upper):
    low, high = jnp.split(value, 2, axis=0)
    return jnp.where(upper, high, low), jnp.where(upper, low, high)


def carried_states(forward, backward, decay, together):
    chips = lax.axis_size("chip")
    upper = lax.axis_index("core") == 1
    heads, head_size, _ = forward.shape
    share = heads // (2 * PARTS * chips)
    rows = share * head_size
    high = decay.astype(BF16)
    low = (decay - high.astype(F32)).astype(BF16)

    def parted(v):
        return v.reshape(PARTS, chips, share, *v.shape[1:])

    own_forward, their_forward = halves(forward.astype(BF16), upper)
    own_backward, their_backward = halves(backward.astype(BF16), upper)
    own_decay, _ = halves(decay, upper)
    wide = jnp.broadcast_to(jnp.stack([high, low], axis=1)[:, :, None], (heads, 2, STATE))
    _, their_wide = halves(wide, upper)
    sent = jnp.concatenate(
        [v.reshape(-1, STATE) for v in (their_forward, their_backward, their_wide)]
    )
    got = core_swap(sent)
    size = heads // 2 * head_size
    got_forward = got[:size].reshape(own_forward.shape)
    got_backward = got[size : 2 * size].reshape(own_forward.shape)
    got_decay = jnp.sum(got[2 * size :].reshape(heads // 2, 2, STATE)[:, :, 0].astype(F32), axis=1)
    forward_0 = jnp.where(upper, got_forward, own_forward)
    forward_1 = jnp.where(upper, own_forward, got_forward)
    backward_0 = jnp.where(upper, got_backward, own_backward)
    backward_1 = jnp.where(upper, own_backward, got_backward)
    decay_0 = jnp.where(upper, got_decay, own_decay)[:, None, None]
    decay_1 = jnp.where(upper, own_decay, got_decay)[:, None, None]
    chip_forward = parted((forward_1 + decay_1 * forward_0).astype(BF16))
    chip_backward = parted((backward_0 + decay_0 * backward_1).astype(BF16))
    chip_decay = (decay_0 * decay_1)[:, 0, 0]
    high = chip_decay.astype(BF16)
    low = (chip_decay - high.astype(F32)).astype(BF16)
    wide = parted(jnp.broadcast_to(jnp.stack([high, low], axis=1)[:, :, None], (heads // 2, 2, STATE)))

    def trade(tiles):
        return lax.all_to_all(tiles, "chip", 0, 0, tiled=True)

    arrived = [
        trade(
            jnp.concatenate(
                [v[part].reshape(chips, -1, STATE) for v in (chip_forward, chip_backward, wide)],
                axis=1,
            )
        )
        for part in range(PARTS)
    ]
    arrived[0] = together(arrived[0])
    states = []
    for part in range(PARTS):
        tiles = arrived[part]
        shape = (chips, share, head_size, STATE)
        terms = tiles[:, :rows].reshape(shape).astype(F32)
        back = tiles[:, rows : 2 * rows].reshape(shape).astype(F32)
        factor = jnp.sum(
            tiles[:, 2 * rows :].reshape(chips, share, 2, STATE).astype(F32), axis=2
        )[:, :, None, :]
        entries, laters = [jnp.zeros(shape[1:], F32)], [jnp.zeros(shape[1:], F32)]
        for i in range(chips - 1):
            entries.append(terms[i] + factor[i] * entries[-1])
            k = chips - 1 - i
            laters.append(back[k] + factor[k] * laters[-1])
        pair = jnp.stack([jnp.stack(entries), jnp.stack(laters[::-1])], axis=1)
        states.append(trade(pair.astype(BF16).reshape(chips, 2 * rows, STATE)))
    results = []

    def of_part(v, part):
        return v.reshape(PARTS, -1, *v.shape[1:])[part]

    for part in range(PARTS):
        tiles = states[part].reshape(chips, 2, share, head_size, STATE)
        entry = tiles[:, 0].reshape(chips * share, head_size, STATE)
        later = tiles[:, 1].reshape(chips * share, head_size, STATE)
        entry_1 = (of_part(forward_0, part) + of_part(decay_0, part) * entry).astype(BF16)
        later_0 = (of_part(backward_1, part) + of_part(decay_1, part) * later).astype(BF16)
        mine = jnp.stack([jnp.where(upper, entry_1, entry), jnp.where(upper, later, later_0)])
        theirs = jnp.stack([jnp.where(upper, entry, entry_1), jnp.where(upper, later_0, later)])
        other = core_swap(theirs)
        results.append(
            jnp.stack([jnp.where(upper, other, mine), jnp.where(upper, mine, other)], axis=1)
        )
    return results


def body(
    layer_input, dt_weight, dt_bias, decay_rate, ssm_input, in_basis, out_basis, out_cotangent
):
    tokens = layer_input[0]
    length = tokens.shape[0]
    heads = dt_weight.shape[1]
    groups = in_basis.shape[2] // STATE
    per_group = heads // groups
    head_size = ssm_input.shape[2] // heads
    raw = jnp.dot(tokens, gathered_rows(dt_weight), preferred_element_type=F32) + dt_bias
    step_size = jax.nn.softplus(raw)
    rate_grid = decay_rate.reshape(groups, per_group)
    step_grid = step_size.reshape(length, groups, per_group)
    position = jnp.arange(length)
    lower = position[:, None] >= position[None, :]
    cumulative = jnp.dot(
        lower.astype(F32), -decay_rate * step_size, precision=HIGH
    ).reshape(length, groups, per_group)
    final = cumulative[-1]
    tail = jnp.exp(final[None] - cumulative)
    leading = jnp.exp(cumulative)
    inputs_half = ssm_input[0].reshape(length, groups, per_group, head_size)
    upstream_half = out_cotangent[0].reshape(length, groups, per_group, head_size)
    bin_half = in_basis[0].reshape(length, groups, STATE)
    bout_half = out_basis[0].reshape(length, groups, STATE)
    inputs = inputs_half.astype(F32)
    upstream = upstream_half.astype(F32)
    tailed = ((tail * step_grid)[..., None] * inputs).astype(BF16)
    led = (leading[..., None] * upstream).astype(BF16)
    local_state = jnp.einsum("sgkp,sgn->gkpn", tailed, bin_half, preferred_element_type=F32)
    local_grad = jnp.einsum("tgkp,tgn->gkpn", led, bout_half, preferred_element_type=F32)
    cum_rows = cumulative.transpose(1, 2, 0)
    spread = cum_rows[:, :, :, None] - cum_rows[:, :, None, :]
    decay_mat = jnp.where(lower, jnp.exp(jnp.where(lower, spread, 0.0)), 0.0)
    intersection = jnp.einsum("tgn,sgn->gts", bout_half, bin_half, preferred_element_type=F32)
    weighted = (decay_mat * intersection[:, None]).astype(BF16)
    step_cols = step_grid.transpose(1, 2, 0)[:, :, None, :]
    pair = jnp.einsum("tgkp,sgkp->gkts", upstream_half, inputs_half, preferred_element_type=F32)
    through = jnp.einsum("gkts,tgkp->sgkp", weighted, upstream_half, preferred_element_type=F32)
    scaled = decay_mat * pair * step_cols
    joint = jnp.sum(scaled, axis=1).astype(BF16)
    moment = scaled * intersection[:, None]
    change = (jnp.sum(moment, axis=-1) - jnp.sum(moment, axis=-2)).transpose(2, 0, 1)
    local_b = jnp.einsum("gts,tgn->sgn", joint, bout_half, preferred_element_type=F32)
    local_c = jnp.einsum("gts,sgn->tgn", joint, bin_half, preferred_element_type=F32)

    fixed = {}

    def together(got):
        got, *rest = lax.optimization_barrier((got, through, change, local_b, local_c))
        fixed["local"] = rest
        return got

    flat = (heads, head_size, STATE)
    parts = carried_states(
        local_state.reshape(flat), local_grad.reshape(flat), jnp.exp(final).reshape(heads), together
    )
    through, change, local_b, local_c = fixed["local"]
    grads_x, grads_b, grads_c, grads_step = [], [], [], []
    for part in range(PARTS):
        picked = slice(part, None, PARTS)
        entry, later = (
            v.reshape(groups // PARTS, per_group, head_size, STATE) for v in parts[part]
        )
        x, dy = inputs[:, picked], upstream[:, picked]
        steps, tails, leads = step_grid[:, picked], tail[:, picked], leading[:, picked]
        carried = jnp.einsum("sgn,gkpn->sgkp", bin_half[:, picked], later, preferred_element_type=F32)
        read = jnp.einsum("tgn,gkpn->tgkp", bout_half[:, picked], entry, preferred_element_type=F32)
        inner_x = through[:, picked] + tails[..., None] * carried
        direct = jnp.sum(x * inner_x, axis=-1)
        entry_term = leads * jnp.sum(read * dy, axis=-1)
        exit_term = tails * steps * jnp.sum(x * carried, axis=-1)
        closing = jnp.exp(final[picked]) * jnp.sum(
            later.astype(F32) * entry.astype(F32), axis=(2, 3)
        ) + jnp.sum(exit_term, axis=0)
        grad_cum = change[:, picked] + entry_term - exit_term
        grad_log = jnp.einsum("ut,ugk->tgk", lower.astype(F32), grad_cum, precision=HIGH) + closing
        grads_step.append(direct - rate_grid[picked] * grad_log)
        grads_x.append(steps[..., None] * inner_x)
        grads_b.append(
            local_b[:, picked]
            + jnp.einsum("sgkp,gkpn->sgn", tailed[:, picked], later, preferred_element_type=F32)
        )
        grads_c.append(
            local_c[:, picked]
            + jnp.einsum("tgkp,gkpn->tgn", led[:, picked], entry, preferred_element_type=F32)
        )

    def whole(pieces):
        shape = pieces[0].shape
        return jnp.stack(pieces, axis=2).reshape(shape[0], groups, *shape[2:])

    grad_raw = whole(grads_step).reshape(length, heads) * jax.nn.sigmoid(raw)
    partial = lax.dot_general(
        tokens, grad_raw.astype(BF16), (((0,), (0,)), ((), ())), preferred_element_type=F32
    )
    grad_weight = summed_rows(partial)
    out_x = whole(grads_x).reshape(1, length, heads * head_size).astype(BF16)
    out_b = whole(grads_b).reshape(1, length, groups * STATE).astype(BF16)
    out_c = whole(grads_c).reshape(1, length, groups * STATE).astype(BF16)
    return (out_x, out_b, out_c, grad_weight)


def solution(mesh):
    blocks = mesh.shape["seq"]
    split = Mesh(
        mesh.devices.reshape(mesh.shape["fsdp"], blocks // CORES, CORES), ("fsdp", *SEQ)
    )
    wide = P("fsdp", SEQ, None)
    return jax.shard_map(
        body,
        mesh=split,
        in_specs=(wide, P("fsdp", None), P(), P(), wide, wide, wide, wide),
        out_specs=(wide, wide, wide, P("fsdp", None)),
        check_vma=False,
    )
```

```python
import jax
import jax.numpy as jnp
from jax import lax
from jax.sharding import Mesh
from jax.sharding import PartitionSpec as P

STATE = 128
LANES = 128
CORES = 2
SEQ = ("chip", "core")

HIGH = lax.Precision.HIGHEST
F32 = jnp.float32
BF16 = jnp.bfloat16


def core_swap(value):
    return lax.ppermute(value, "core", [(0, 1), (1, 0)])


def copies_to(value, axis):
    tiles = jnp.broadcast_to(value[None], (lax.axis_size(axis), *value.shape))
    return lax.all_to_all(tiles, axis, 0, 0, tiled=True)


def packed_rows(rows, packs):
    return jnp.concatenate(jnp.split(rows, packs, axis=0), axis=1)


def carried_states(forward, backward, decay, together):
    chips = lax.axis_size("chip")
    heads, head_size, _ = forward.shape
    share = heads // chips
    rows = share * head_size
    high = decay.astype(BF16)
    low = (decay - high.astype(F32)).astype(BF16)
    wide = jnp.broadcast_to(jnp.stack([high, low], axis=1)[:, :, None], (heads, 2, STATE))
    tiles = jnp.concatenate(
        [v.astype(BF16).reshape(chips, -1, STATE) for v in (forward, backward, wide)], axis=1
    )
    tiles = together(lax.all_to_all(tiles, "chip", 0, 0, tiled=True))
    shape = (chips, share, head_size, STATE)
    terms = tiles[:, :rows].reshape(shape).astype(F32)
    back = tiles[:, rows : 2 * rows].reshape(shape).astype(F32)
    factor = jnp.sum(tiles[:, 2 * rows :].reshape(chips, share, 2, STATE).astype(F32), axis=2)
    factor = factor[:, :, None, :]
    entries, laters = [jnp.zeros(shape[1:], F32)], [jnp.zeros(shape[1:], F32)]
    for i in range(chips - 1):
        entries.append(terms[i] + factor[i] * entries[-1])
        k = chips - 1 - i
        laters.append(back[k] + factor[k] * laters[-1])
    pair = jnp.stack([jnp.stack(entries), jnp.stack(laters[::-1])], axis=1)
    tiles = pair.astype(BF16).reshape(chips, 2 * rows, STATE)
    tiles = lax.all_to_all(tiles, "chip", 0, 0, tiled=True)
    return tiles[:, :rows].reshape(forward.shape), tiles[:, rows:].reshape(forward.shape)


def body(
    layer_input, dt_weight, dt_bias, decay_rate, ssm_input, in_basis, out_basis, out_cotangent
):
    upper = lax.axis_index("core") == 1

    def picked(v, own):
        low, high = jnp.split(v, CORES, axis=-1)
        return jnp.where(upper == own, high, low)

    def in_order(own, other):
        return jnp.where(upper, jnp.stack([other, own]), jnp.stack([own, other]))

    tokens = layer_input[0]
    length, width = tokens.shape
    heads = dt_weight.shape[1] // CORES
    groups = in_basis.shape[2] // STATE // CORES
    per_group = heads // groups
    head_size = ssm_input.shape[2] // CORES // heads
    packs = LANES // heads
    rows = dt_weight.shape[0] // packs
    devices = lax.axis_size("fsdp")

    weight = copies_to(packed_rows(picked(dt_weight, True), packs), "fsdp")
    weight = weight.reshape(width // packs, LANES)
    both_tokens = jnp.stack([tokens, core_swap(tokens)]).reshape(CORES * length, width)
    sides = (ssm_input[0], out_cotangent[0], in_basis[0], out_basis[0])
    cuts = [0]
    for side in sides:
        cuts.append(cuts[-1] + side.shape[1] // CORES)
    other_sides = core_swap(jnp.concatenate([picked(side, False) for side in sides], axis=1))
    x_half, dy_half, bin_half, bout_half = (
        in_order(picked(side, True), other_sides[:, cuts[i] : cuts[i + 1]])
        for i, side in enumerate(sides)
    )
    bias, rate = picked(dt_bias, True), picked(decay_rate, True)

    chunk = LANES * packs
    near = rows * packs
    target = jnp.arange(chunk)
    pack, place = target // LANES, target % LANES
    source = place // rows * near + pack * rows + place % rows
    order = (jnp.arange(chunk)[:, None] == source[None, :]).astype(BF16)
    columns = jnp.einsum(
        "pgc,cad->apgd",
        both_tokens.reshape(CORES * length, width // chunk, chunk),
        order.reshape(chunk, packs, LANES),
        preferred_element_type=BF16,
    ).reshape(packs, CORES * length, width // packs)

    product = jnp.einsum("apk,km->apm", columns, weight, preferred_element_type=F32)
    raw = bias + sum(product[a, :, a * heads : (a + 1) * heads] for a in range(packs))
    raw = in_order(raw[:length], raw[length:])
    step_size = jax.nn.softplus(raw)
    position = jnp.arange(length)
    lower = position[:, None] >= position[None, :]
    triangle = lower.astype(F32)
    cumulative = jnp.einsum("tu,buh->bth", triangle, -rate * step_size, precision=HIGH)
    grid = (CORES, length, groups, per_group)
    final = cumulative[:, -1].reshape(CORES, groups, per_group)
    cumulative = cumulative.reshape(grid)
    step_grid = step_size.reshape(grid)
    rate_grid = rate.reshape(groups, per_group)
    tail = jnp.exp(final[:, None] - cumulative)
    leading = jnp.exp(cumulative)
    block_decay = jnp.exp(final)
    x_half = x_half.reshape(*grid, head_size)
    dy_half = dy_half.reshape(*grid, head_size)
    bin_half = bin_half.reshape(CORES, length, groups, STATE)
    bout_half = bout_half.reshape(CORES, length, groups, STATE)
    inputs = x_half.astype(F32)
    upstream = dy_half.astype(F32)
    tailed = ((tail * step_grid)[..., None] * inputs).astype(BF16)
    led = (leading[..., None] * upstream).astype(BF16)
    forward = jnp.einsum("bsgkp,bsgn->bgkpn", tailed, bin_half, preferred_element_type=F32)
    backward = jnp.einsum("btgkp,btgn->bgkpn", led, bout_half, preferred_element_type=F32)
    factor = block_decay[..., None, None]
    chip_forward = forward[1] + factor[1] * forward[0]
    chip_backward = backward[0] + factor[0] * backward[1]

    cum_rows = cumulative.transpose(0, 2, 3, 1)
    spread = cum_rows[..., :, None] - cum_rows[..., None, :]
    decay_mat = jnp.where(lower, jnp.exp(jnp.where(lower, spread, 0.0)), 0.0)
    intersection = jnp.einsum("btgn,bsgn->bgts", bout_half, bin_half, preferred_element_type=F32)
    weighted = (decay_mat * intersection[:, :, None]).astype(BF16)
    step_cols = step_grid.transpose(0, 2, 3, 1)[..., None, :]
    pair = jnp.einsum("btgkp,bsgkp->bgkts", dy_half, x_half, preferred_element_type=F32)
    through = jnp.einsum("bgkts,btgkp->bsgkp", weighted, dy_half, preferred_element_type=F32)
    scaled = decay_mat * pair * step_cols
    joint = jnp.sum(scaled, axis=2).astype(BF16)
    moment = scaled * intersection[:, :, None]
    change = (jnp.sum(moment, axis=-1) - jnp.sum(moment, axis=-2)).transpose(0, 3, 1, 2)
    local_b = jnp.einsum("bgts,btgn->bsgn", joint, bout_half, preferred_element_type=F32)
    local_c = jnp.einsum("bgts,bsgn->btgn", joint, bin_half, preferred_element_type=F32)
    local = [through, change, local_b, local_c]

    def together(got):
        got, *local[:] = lax.optimization_barrier((got, *local))
        return got

    flat = (heads, head_size, STATE)
    entry, later = carried_states(
        chip_forward.reshape(flat),
        chip_backward.reshape(flat),
        (block_decay[0] * block_decay[1]).reshape(heads),
        together,
    )
    through, change, local_b, local_c = local
    entry = entry.reshape(forward.shape[1:])
    later = later.reshape(forward.shape[1:])
    entry = jnp.stack([entry, (forward[0] + factor[0] * entry).astype(BF16)])
    later = jnp.stack([(backward[1] + factor[1] * later).astype(BF16), later])

    carried = jnp.einsum("bsgn,bgkpn->bsgkp", bin_half, later, preferred_element_type=F32)
    read = jnp.einsum("btgn,bgkpn->btgkp", bout_half, entry, preferred_element_type=F32)
    inner_x = through + tail[..., None] * carried
    direct = jnp.sum(inputs * inner_x, axis=-1)
    entry_term = leading * jnp.sum(read * upstream, axis=-1)
    exit_term = tail * step_grid * jnp.sum(inputs * carried, axis=-1)
    closing = block_decay * jnp.sum(
        later.astype(F32) * entry.astype(F32), axis=(3, 4)
    ) + jnp.sum(exit_term, axis=1)
    grad_cum = change + entry_term - exit_term
    grad_log = jnp.einsum("ut,bugk->btgk", triangle, grad_cum, precision=HIGH) + closing[:, None]
    grad_step = direct - rate_grid * grad_log
    grad_raw = grad_step.reshape(raw.shape) * jax.nn.sigmoid(raw)

    grad_raw = jnp.where(upper, grad_raw[::-1], grad_raw).astype(BF16)
    grad_raw = grad_raw.reshape(CORES * length, heads)
    placed = jnp.eye(packs, dtype=BF16)[:, None, :, None] * grad_raw[None, :, None, :]
    placed = placed.reshape(packs, CORES * length, LANES)
    partial = jnp.einsum("apk,apm->km", columns, placed, preferred_element_type=F32)
    tiles = partial.astype(BF16).reshape(devices, rows, LANES)
    tiles = lax.all_to_all(tiles, "fsdp", 0, 0, tiled=True)

    grad_x = (step_grid[..., None] * inner_x).astype(BF16)
    grad_b = local_b + jnp.einsum("bsgkp,bgkpn->bsgn", tailed, later, preferred_element_type=F32)
    grad_c = local_c + jnp.einsum("btgkp,bgkpn->btgn", led, entry, preferred_element_type=F32)
    outs = jnp.concatenate(
        [v.astype(BF16).reshape(CORES, length, -1) for v in (grad_x, grad_b, grad_c)], axis=2
    )
    tiles, outs = lax.optimization_barrier((tiles, outs))
    own_outs = jnp.where(upper, outs[1], outs[0])
    other_outs = core_swap(jnp.where(upper, outs[0], outs[1]))
    own_rows = jnp.sum(tiles.astype(F32), axis=0)
    blocks = copies_to(own_rows, SEQ).reshape(-1, CORES, rows, packs, heads)
    grad_weight = jnp.sum(blocks, axis=0).transpose(2, 1, 0, 3).reshape(dt_weight.shape)

    def joined(first, last):
        own, other = own_outs[:, first:last], other_outs[:, first:last]
        low, high = jnp.where(upper, other, own), jnp.where(upper, own, other)
        return jnp.concatenate([low, high], axis=1)[None]

    out_x, out_b, out_c = (
        joined(first, last)
        for first, last in ((0, cuts[1]), (cuts[1], cuts[1] + groups * STATE), (cuts[1] + groups * STATE, outs.shape[2]))
    )
    return (out_x, out_b, out_c, grad_weight)


def solution(mesh):
    blocks = mesh.shape["seq"]
    split = Mesh(
        mesh.devices.reshape(mesh.shape["fsdp"], blocks // CORES, CORES), ("fsdp", *SEQ)
    )
    wide = P("fsdp", SEQ, None)
    return jax.shard_map(
        body,
        mesh=split,
        in_specs=(wide, P("fsdp", None), P(), P(), wide, wide, wide, wide),
        out_specs=(wide, wide, wide, P("fsdp", None)),
        check_vma=False,
    )
```

```python
import jax
import jax.numpy as jnp
from jax import lax
from jax.sharding import Mesh
from jax.sharding import PartitionSpec as P


STATE = 128
LANES = 128
CORES = 2
SEQ = ("chip", "core")

HIGH = lax.Precision.HIGHEST
F32 = jnp.float32
BF16 = jnp.bfloat16


def core_swap(value):
    return lax.ppermute(value, "core", [(0, 1), (1, 0)])


def copies_to(value, axis):
    tiles = jnp.broadcast_to(value[None], (lax.axis_size(axis), *value.shape))
    return lax.all_to_all(tiles, axis, 0, 0, tiled=True)


def packed_rows(rows, packs):
    return jnp.concatenate(jnp.split(rows, packs, axis=0), axis=1)


def carried_states(forward, backward, decay, together):
    chips = lax.axis_size("chip")
    heads, head_size, _ = forward.shape
    share = heads // chips
    rows = share * head_size
    high = decay.astype(BF16)
    low = (decay - high.astype(F32)).astype(BF16)
    wide = jnp.broadcast_to(jnp.stack([high, low], axis=1)[:, :, None], (heads, 2, STATE))
    tiles = jnp.concatenate(
        [v.astype(BF16).reshape(chips, -1, STATE) for v in (forward, backward, wide)], axis=1
    )
    tiles = together(lax.all_to_all(tiles, "chip", 0, 0, tiled=True))
    shape = (chips, share, head_size, STATE)
    terms = tiles[:, :rows].reshape(shape).astype(F32)
    back = tiles[:, rows : 2 * rows].reshape(shape).astype(F32)
    factor = jnp.sum(tiles[:, 2 * rows :].reshape(chips, share, 2, STATE).astype(F32), axis=2)
    factor = factor[:, :, None, :]
    entries, laters = [jnp.zeros(shape[1:], F32)], [jnp.zeros(shape[1:], F32)]
    for i in range(chips - 1):
        entries.append(terms[i] + factor[i] * entries[-1])
        k = chips - 1 - i
        laters.append(back[k] + factor[k] * laters[-1])
    pair = jnp.stack([jnp.stack(entries), jnp.stack(laters[::-1])], axis=1)
    tiles = pair.astype(BF16).reshape(chips, 2 * rows, STATE)
    tiles = lax.all_to_all(tiles, "chip", 0, 0, tiled=True)
    return tiles[:, :rows].reshape(forward.shape), tiles[:, rows:].reshape(forward.shape)


def body(
    layer_input, dt_weight, dt_bias, decay_rate, ssm_input, in_basis, out_basis, out_cotangent
):
    upper = lax.axis_index("core") == 1

    def chosen(v, own):
        return jnp.where(upper == own, v[1], v[0])

    def in_order(own, other):
        return jnp.where(upper, jnp.stack([other, own]), jnp.stack([own, other]))

    tokens = layer_input[0]
    length, width = tokens.shape
    heads = dt_weight.shape[1] // CORES
    groups = in_basis.shape[2] // STATE // CORES
    per_group = heads // groups
    head_size = ssm_input.shape[2] // CORES // heads
    packs = LANES // heads
    rows = dt_weight.shape[0] // packs
    devices = lax.axis_size("fsdp")

    weight_half = chosen(jnp.stack(jnp.split(dt_weight, CORES, axis=1)), True)
    weight = copies_to(packed_rows(weight_half, packs), "fsdp").reshape(width // packs, LANES)
    both_tokens = jnp.stack([tokens, core_swap(tokens)]).reshape(CORES * length, width)

    def by_group(basis):
        return jnp.stack(jnp.split(basis, CORES * groups, axis=1)).reshape(CORES, -1, STATE)

    sides = [v[0].T.reshape(CORES, -1, length) for v in (ssm_input, out_cotangent)]
    sides += [by_group(v[0]) for v in (in_basis, out_basis)]
    cuts = [0]
    for side in sides:
        cuts.append(cuts[-1] + side.shape[1])
    other_sides = core_swap(jnp.concatenate([chosen(side, False) for side in sides]))
    x_half, dy_half, bin_half, bout_half = (
        in_order(chosen(side, True), other_sides[cuts[i] : cuts[i + 1]])
        for i, side in enumerate(sides)
    )
    bias, rate = (
        chosen(v.reshape(CORES, heads, 1), True) for v in (dt_bias, decay_rate)
    )

    chunk = LANES * packs
    near = rows * packs
    target = jnp.arange(chunk)
    pack, place = target // LANES, target % LANES
    source = place // rows * near + pack * rows + place % rows
    order = (jnp.arange(chunk)[:, None] == source[None, :]).astype(BF16)
    columns = jnp.einsum(
        "pgc,cad->agdp",
        both_tokens.reshape(CORES * length, width // chunk, chunk),
        order.reshape(chunk, packs, LANES),
        preferred_element_type=BF16,
    ).reshape(packs, width // packs, CORES * length)

    product = jnp.einsum("akp,km->amp", columns, weight, preferred_element_type=F32)
    raw = bias + sum(product[a, a * heads : (a + 1) * heads] for a in range(packs))
    raw = in_order(raw[:, :length], raw[:, length:])
    step_size = jax.nn.softplus(raw)
    position = jnp.arange(length)
    lower = position[:, None] >= position[None, :]
    triangle = lower.astype(F32)
    cumulative = jnp.einsum("bhu,tu->bht", -rate * step_size, triangle, precision=HIGH)
    grid = (CORES, groups, per_group, length)
    cumulative = cumulative.reshape(grid)
    final = cumulative[..., -1:]
    step_grid = step_size.reshape(grid)
    tail = jnp.exp(final - cumulative)
    leading = jnp.exp(cumulative)
    block_decay = jnp.exp(final)
    x_half = x_half.reshape(CORES, groups, per_group, head_size, length)
    dy_half = dy_half.reshape(x_half.shape)
    bin_half = bin_half.reshape(CORES, groups, length, STATE)
    bout_half = bout_half.reshape(bin_half.shape)
    inputs = x_half.astype(F32)
    upstream = dy_half.astype(F32)
    tailed = ((tail * step_grid)[..., None, :] * inputs).astype(BF16)
    led = (leading[..., None, :] * upstream).astype(BF16)
    forward = jnp.einsum("bgkps,bgsn->bgkpn", tailed, bin_half, preferred_element_type=F32)
    backward = jnp.einsum("bgkpt,bgtn->bgkpn", led, bout_half, preferred_element_type=F32)
    factor = block_decay[..., None]
    chip_forward = forward[1] + factor[1] * forward[0]
    chip_backward = backward[0] + factor[0] * backward[1]

    spread = cumulative[..., :, None] - cumulative[..., None, :]
    decay_mat = jnp.where(lower, jnp.exp(jnp.where(lower, spread, 0.0)), 0.0)
    intersection = jnp.einsum("bgtn,bgsn->bgts", bout_half, bin_half, preferred_element_type=F32)
    weighted = (decay_mat * intersection[:, :, None]).astype(BF16)
    pair = jnp.einsum("bgkpt,bgkps->bgkts", dy_half, x_half, preferred_element_type=F32)
    through = jnp.einsum("bgkpt,bgkts->bgkps", dy_half, weighted, preferred_element_type=F32)
    scaled = decay_mat * pair * step_grid[..., None, :]
    joint = jnp.sum(scaled, axis=2).astype(BF16)
    moment = scaled * intersection[:, :, None]
    change = jnp.sum(moment, axis=-1) - jnp.sum(moment, axis=-2)
    local_b = jnp.einsum("bgts,bgtn->bgsn", joint, bout_half, preferred_element_type=F32)
    local_c = jnp.einsum("bgts,bgsn->bgtn", joint, bin_half, preferred_element_type=F32)
    local = [through, change, local_b, local_c]

    def together(got):
        got, *local[:] = lax.optimization_barrier((got, *local))
        return got

    flat = (heads, head_size, STATE)
    entry, later = carried_states(
        chip_forward.reshape(flat),
        chip_backward.reshape(flat),
        (block_decay[0] * block_decay[1]).reshape(heads),
        together,
    )
    through, change, local_b, local_c = local
    entry = entry.reshape(forward.shape[1:])
    later = later.reshape(forward.shape[1:])
    entry = jnp.stack([entry, (forward[0] + factor[0] * entry).astype(BF16)])
    later = jnp.stack([(backward[1] + factor[1] * later).astype(BF16), later])

    carried = jnp.einsum("bgkpn,bgsn->bgkps", later, bin_half, preferred_element_type=F32)
    read = jnp.einsum("bgkpn,bgtn->bgkpt", entry, bout_half, preferred_element_type=F32)
    inner_x = through + tail[..., None, :] * carried
    direct = jnp.sum(inputs * inner_x, axis=3)
    entry_term = leading * jnp.sum(read * upstream, axis=3)
    exit_term = tail * step_grid * jnp.sum(inputs * carried, axis=3)
    closing = block_decay[..., 0] * jnp.sum(
        later.astype(F32) * entry.astype(F32), axis=(3, 4)
    ) + jnp.sum(exit_term, axis=-1)
    grad_cum = (change + entry_term - exit_term).reshape(CORES * heads, length)
    grad_log = jnp.dot(grad_cum, triangle, precision=HIGH).reshape(grid) + closing[..., None]
    grad_step = direct - rate.reshape(groups, per_group, 1) * grad_log
    grad_raw = grad_step.reshape(raw.shape) * jax.nn.sigmoid(raw)

    grad_raw = jnp.where(upper, grad_raw[::-1], grad_raw).astype(BF16)
    grad_raw = jnp.concatenate([grad_raw[0], grad_raw[1]], axis=1)
    zero = jnp.zeros_like(grad_raw)
    placed = jnp.stack(
        [jnp.concatenate([grad_raw if i == a else zero for i in range(packs)]) for a in range(packs)]
    )
    partial = jnp.einsum("akp,amp->km", columns, placed, preferred_element_type=F32)
    tiles = partial.astype(BF16).reshape(devices, rows, LANES)
    tiles = lax.all_to_all(tiles, "fsdp", 0, 0, tiled=True)

    grad_x = (step_grid[..., None, :] * inner_x).astype(BF16)
    grad_b = jnp.einsum("bgkps,bgkpn->bgsn", tailed, later, preferred_element_type=F32)
    grad_b = (local_b + grad_b).astype(BF16)
    grad_c = jnp.einsum("bgkpt,bgkpn->bgtn", led, entry, preferred_element_type=F32)
    grad_c = (local_c + grad_c).astype(BF16)
    outs = jnp.concatenate(
        [v.reshape(CORES, -1, LANES) for v in (grad_x, grad_b, grad_c)], axis=1
    )
    own_outs = chosen(outs, True)
    other_outs = core_swap(chosen(outs, False))

    def joined(first, last):
        return in_order(own_outs[first:last], other_outs[first:last])

    size, basis = heads * head_size, groups * length
    out_x = joined(0, size).reshape(CORES * size, length).T
    outs_bc = []
    for first in (size, size + basis):
        whole = joined(first, first + basis).reshape(CORES * groups, length, STATE)
        outs_bc.append(jnp.concatenate([whole[g] for g in range(CORES * groups)], axis=1)[None])
    own_rows = jnp.sum(tiles.astype(F32), axis=0)
    blocks = copies_to(own_rows, SEQ).reshape(-1, CORES, rows, packs, heads)
    grad_weight = jnp.sum(blocks, axis=0).transpose(2, 1, 0, 3).reshape(dt_weight.shape)
    return (out_x[None], *outs_bc, grad_weight)


def solution(mesh):
    blocks = mesh.shape["seq"]
    split = Mesh(
        mesh.devices.reshape(mesh.shape["fsdp"], blocks // CORES, CORES), ("fsdp", *SEQ)
    )
    wide = P("fsdp", SEQ, None)
    return jax.shard_map(
        body,
        mesh=split,
        in_specs=(wide, P("fsdp", None), P(), P(), wide, wide, wide, wide),
        out_specs=(wide, wide, wide, P("fsdp", None)),
        check_vma=False,
    )
```

```python
import jax
import jax.numpy as jnp
from jax import lax
from jax.sharding import Mesh
from jax.sharding import PartitionSpec as P


STATE = 128
LANES = 128
CORES = 2
SEQ = ("chip", "core")

HIGH = lax.Precision.HIGHEST
F32 = jnp.float32
BF16 = jnp.bfloat16


def core_swap(value):
    return lax.ppermute(value, "core", [(0, 1), (1, 0)])


def copies_to(value, axis):
    tiles = jnp.broadcast_to(value[None], (lax.axis_size(axis), *value.shape))
    return lax.all_to_all(tiles, axis, 0, 0, tiled=True)


def packed_rows(rows, packs):
    return jnp.concatenate(jnp.split(rows, packs, axis=0), axis=1)


def carried_states(forward, backward, decay, together):
    chips = lax.axis_size("chip")
    heads, head_size, _ = forward.shape
    share = heads // chips
    rows = share * head_size
    wide = jnp.broadcast_to(decay[:, None], (heads, STATE))
    high = wide.astype(BF16)
    low = wide - high.astype(F32)
    tiles = jnp.concatenate(
        [v.astype(BF16).reshape(chips, -1, STATE) for v in (forward, backward, high, low)], axis=1
    )
    tiles = together(lax.all_to_all(tiles, "chip", 0, 0, tiled=True))
    shape = (chips, share, head_size, STATE)
    terms = tiles[:, :rows].reshape(shape).astype(F32)
    back = tiles[:, rows : 2 * rows].reshape(shape).astype(F32)
    factors = tiles[:, 2 * rows :].astype(F32)
    factor = (factors[:, :share] + factors[:, share:])[:, :, None, :]
    entries, laters = [jnp.zeros(shape[1:], F32)], [jnp.zeros(shape[1:], F32)]
    for i in range(chips - 1):
        entries.append(terms[i] + factor[i] * entries[-1])
        k = chips - 1 - i
        laters.append(back[k] + factor[k] * laters[-1])
    pair = jnp.stack([jnp.stack(entries), jnp.stack(laters[::-1])], axis=1)
    tiles = pair.astype(BF16).reshape(chips, 2 * rows, STATE)
    tiles = lax.all_to_all(tiles, "chip", 0, 0, tiled=True)
    return tiles[:, :rows].reshape(forward.shape), tiles[:, rows:].reshape(forward.shape)


def body(
    layer_input, dt_weight, dt_bias, decay_rate, ssm_input, in_basis, out_basis, out_cotangent
):
    upper = lax.axis_index("core") == 1

    def chosen(v, own):
        return jnp.where(upper == own, v[1], v[0])

    def in_order(own, other):
        return jnp.where(upper, jnp.stack([other, own]), jnp.stack([own, other]))

    tokens = layer_input[0]
    length, width = tokens.shape
    heads = dt_weight.shape[1] // CORES
    groups = in_basis.shape[2] // STATE // CORES
    per_group = heads // groups
    head_size = ssm_input.shape[2] // CORES // heads
    packs = LANES // heads
    rows = dt_weight.shape[0] // packs
    devices = lax.axis_size("fsdp")

    weight_half = chosen(jnp.stack(jnp.split(dt_weight, CORES, axis=1)), True)
    weight = copies_to(packed_rows(weight_half, packs), "fsdp").reshape(width // packs, LANES)
    both_tokens = jnp.stack([tokens, core_swap(tokens)]).reshape(CORES * length, width)

    sides = [v[0] for v in (ssm_input, out_cotangent, in_basis, out_basis)]
    cuts = [0]
    for side in sides:
        cuts.append(cuts[-1] + side.shape[1] // CORES)

    def picked(v, own):
        low, high = jnp.split(v, CORES, axis=1)
        return jnp.where(upper == own, high, low)

    other_sides = core_swap(jnp.concatenate([picked(side, False) for side in sides], axis=1))
    x_half, dy_half, bin_half, bout_half = (
        (picked(side, True), other_sides[:, cuts[i] : cuts[i + 1]])
        for i, side in enumerate(sides)
    )

    def tiled(pair):
        return in_order(*(jnp.stack(jnp.split(v, v.shape[1] // LANES, axis=1)) for v in pair))

    unit = jnp.eye(heads * head_size, dtype=BF16)

    def turned(pair):
        return jnp.einsum("bsc,cd->bds", in_order(*pair), unit, preferred_element_type=BF16)

    x_half, dy_half = turned(x_half), turned(dy_half)
    bin_half, bout_half = tiled(bin_half), tiled(bout_half)
    bias, rate = (
        chosen(v.reshape(CORES, heads, 1), True) for v in (dt_bias, decay_rate)
    )

    chunk = LANES * packs
    near = rows * packs
    target = jnp.arange(chunk)
    pack, place = target // LANES, target % LANES
    source = place // rows * near + pack * rows + place % rows
    order = (jnp.arange(chunk)[:, None] == source[None, :]).astype(BF16)
    columns = jnp.einsum(
        "pgc,cad->agdp",
        both_tokens.reshape(CORES * length, width // chunk, chunk),
        order.reshape(chunk, packs, LANES),
        preferred_element_type=BF16,
    ).reshape(packs, width // packs, CORES * length)

    product = jnp.einsum("akp,km->amp", columns, weight, preferred_element_type=F32)
    raw = bias + sum(product[a, a * heads : (a + 1) * heads] for a in range(packs))
    raw = in_order(raw[:, :length], raw[:, length:])
    step_size = jax.nn.softplus(raw)
    position = jnp.arange(length)
    lower = position[:, None] >= position[None, :]
    triangle = lower.astype(F32)
    cumulative = jnp.einsum("bhu,tu->bht", -rate * step_size, triangle, precision=HIGH)
    grid = (CORES, groups, per_group, length)
    cumulative = cumulative.reshape(grid)
    final = cumulative[..., -1:]
    step_grid = step_size.reshape(grid)
    tail = jnp.exp(final - cumulative)
    leading = jnp.exp(cumulative)
    block_decay = jnp.exp(final)
    x_half = x_half.reshape(CORES, groups, per_group, head_size, length)
    dy_half = dy_half.reshape(x_half.shape)
    bin_half = bin_half.reshape(CORES, groups, length, STATE)
    bout_half = bout_half.reshape(bin_half.shape)
    inputs = x_half.astype(F32)
    upstream = dy_half.astype(F32)
    tailed = ((tail * step_grid)[..., None, :] * inputs).astype(BF16)
    led = (leading[..., None, :] * upstream).astype(BF16)
    forward = jnp.einsum("bgkps,bgsn->bgkpn", tailed, bin_half, preferred_element_type=F32)
    backward = jnp.einsum("bgkpt,bgtn->bgkpn", led, bout_half, preferred_element_type=F32)
    factor = block_decay[..., None]
    chip_forward = forward[1] + factor[1] * forward[0]
    chip_backward = backward[0] + factor[0] * backward[1]

    spread = cumulative[..., :, None] - cumulative[..., None, :]
    decay_mat = jnp.where(lower, jnp.exp(jnp.where(lower, spread, 0.0)), 0.0)
    intersection = jnp.einsum("bgtn,bgsn->bgts", bout_half, bin_half, preferred_element_type=F32)
    weighted = (decay_mat * intersection[:, :, None]).astype(BF16)
    pair = jnp.einsum("bgkpt,bgkps->bgkts", dy_half, x_half, preferred_element_type=F32)
    through = jnp.einsum("bgkpt,bgkts->bgkps", dy_half, weighted, preferred_element_type=F32)
    scaled = decay_mat * pair * step_grid[..., None, :]
    joint = jnp.sum(scaled, axis=2).astype(BF16)
    moment = scaled * intersection[:, :, None]
    change = jnp.sum(moment, axis=-1) - jnp.sum(moment, axis=-2)
    local_b = jnp.einsum("bgts,bgtn->bgsn", joint, bout_half, preferred_element_type=F32)
    local_c = jnp.einsum("bgts,bgsn->bgtn", joint, bin_half, preferred_element_type=F32)
    local = [through, change, local_b, local_c]

    def together(got):
        got, *local[:] = lax.optimization_barrier((got, *local))
        return got

    flat = (heads, head_size, STATE)
    entry, later = carried_states(
        chip_forward.reshape(flat),
        chip_backward.reshape(flat),
        jnp.exp(final[0] + final[1]).reshape(heads),
        together,
    )
    through, change, local_b, local_c = local
    entry = entry.reshape(forward.shape[1:])
    later = later.reshape(forward.shape[1:])
    entry = jnp.stack([entry, (forward[0] + factor[0] * entry).astype(BF16)])
    later = jnp.stack([(backward[1] + factor[1] * later).astype(BF16), later])

    carried = jnp.einsum("bgkpn,bgsn->bgkps", later, bin_half, preferred_element_type=F32)
    read = jnp.einsum("bgkpn,bgtn->bgkpt", entry, bout_half, preferred_element_type=F32)
    inner_x = through + tail[..., None, :] * carried
    direct = jnp.sum(inputs * inner_x, axis=3)
    entry_term = leading * jnp.sum(read * upstream, axis=3)
    exit_term = tail * step_grid * jnp.sum(inputs * carried, axis=3)
    closing = block_decay[..., 0] * jnp.sum(
        later.astype(F32) * entry.astype(F32), axis=(3, 4)
    )
    grad_cum = jnp.concatenate([change + entry_term, exit_term], axis=-1)
    sums = jnp.concatenate([triangle, 1.0 - triangle])
    grad_log = jnp.dot(grad_cum.reshape(CORES * heads, -1), sums, precision=HIGH)
    grad_log = grad_log.reshape(grid) + closing[..., None]
    grad_step = direct - rate.reshape(groups, per_group, 1) * grad_log
    grad_raw = grad_step.reshape(raw.shape) * jax.nn.sigmoid(raw)

    grad_raw = jnp.where(upper, grad_raw[::-1], grad_raw).astype(BF16)
    grad_raw = jnp.concatenate([grad_raw[0], grad_raw[1]], axis=1)
    zero = jnp.zeros_like(grad_raw)
    placed = jnp.stack(
        [jnp.concatenate([grad_raw if i == a else zero for i in range(packs)]) for a in range(packs)]
    )
    partial = jnp.einsum("akp,amp->km", columns, placed, preferred_element_type=F32)
    tiles = partial.astype(BF16).reshape(devices, rows, LANES)
    tiles = lax.all_to_all(tiles, "fsdp", 0, 0, tiled=True)

    grad_x = (step_grid[..., None, :] * inner_x).astype(BF16)
    grad_b = jnp.einsum("bgkps,bgkpn->bgsn", tailed, later, preferred_element_type=F32)
    grad_b = (local_b + grad_b).astype(BF16)
    grad_c = jnp.einsum("bgkpt,bgkpn->bgtn", led, entry, preferred_element_type=F32)
    grad_c = (local_c + grad_c).astype(BF16)
    outs = jnp.concatenate(
        [v.reshape(CORES, -1, LANES) for v in (grad_x, grad_b, grad_c)], axis=1
    )
    own_outs = chosen(outs, True)
    other_outs = core_swap(chosen(outs, False))

    def joined(first, last):
        return in_order(own_outs[first:last], other_outs[first:last])

    size, basis = heads * head_size, groups * length
    out_x = joined(0, size).reshape(CORES * size, length).T
    outs_bc = []
    for first in (size, size + basis):
        whole = joined(first, first + basis).reshape(CORES * groups, length, STATE)
        outs_bc.append(jnp.concatenate([whole[g] for g in range(CORES * groups)], axis=1)[None])
    own_rows = jnp.sum(tiles.astype(F32), axis=0)
    blocks = copies_to(own_rows, SEQ).reshape(-1, CORES, rows, packs, heads)
    grad_weight = jnp.sum(blocks, axis=0).transpose(2, 1, 0, 3).reshape(dt_weight.shape)
    return (out_x[None], *outs_bc, grad_weight)


def solution(mesh):
    blocks = mesh.shape["seq"]
    split = Mesh(
        mesh.devices.reshape(mesh.shape["fsdp"], blocks // CORES, CORES), ("fsdp", *SEQ)
    )
    wide = P("fsdp", SEQ, None)
    return jax.shard_map(
        body,
        mesh=split,
        in_specs=(wide, P("fsdp", None), P(), P(), wide, wide, wide, wide),
        out_specs=(wide, wide, wide, P("fsdp", None)),
        check_vma=False,
    )
```

```python
import jax
import jax.numpy as jnp
from jax import lax
from jax.experimental import pallas as pl
from jax.sharding import Mesh
from jax.sharding import PartitionSpec as P


STATE = 128
LANES = 128
CORES = 2
SEQ = ("chip", "core")

HIGH = lax.Precision.HIGHEST
F32 = jnp.float32
BF16 = jnp.bfloat16


def core_swap(value):
    return lax.ppermute(value, "core", [(0, 1), (1, 0)])


def copies_to(value, axis):
    tiles = jnp.broadcast_to(value[None], (lax.axis_size(axis), *value.shape))
    return lax.all_to_all(tiles, axis, 0, 0, tiled=True)


def packed_rows(rows, packs):
    return jnp.concatenate(jnp.split(rows, packs, axis=0), axis=1)


def carried_states(forward, backward, decay, together):
    chips = lax.axis_size("chip")
    heads, head_size, _ = forward.shape
    share = heads // chips
    rows = share * head_size
    wide = jnp.broadcast_to(decay[:, None], (heads, STATE))
    high = wide.astype(BF16)
    low = wide - high.astype(F32)
    tiles = jnp.concatenate(
        [v.astype(BF16).reshape(chips, -1, STATE) for v in (forward, backward, high, low)], axis=1
    )
    tiles = together(lax.all_to_all(tiles, "chip", 0, 0, tiled=True))
    shape = (chips, share, head_size, STATE)
    terms = tiles[:, :rows].reshape(shape).astype(F32)
    back = tiles[:, rows : 2 * rows].reshape(shape).astype(F32)
    factors = tiles[:, 2 * rows :].astype(F32)
    factor = (factors[:, :share] + factors[:, share:])[:, :, None, :]
    entries, laters = [jnp.zeros(shape[1:], F32)], [jnp.zeros(shape[1:], F32)]
    for i in range(chips - 1):
        entries.append(terms[i] + factor[i] * entries[-1])
        k = chips - 1 - i
        laters.append(back[k] + factor[k] * laters[-1])
    pair = jnp.stack([jnp.stack(entries), jnp.stack(laters[::-1])], axis=1)
    tiles = pair.astype(BF16).reshape(chips, 2 * rows, STATE)
    tiles = lax.all_to_all(tiles, "chip", 0, 0, tiled=True)
    return tiles[:, :rows].reshape(forward.shape), tiles[:, rows:].reshape(forward.shape)


def after_trade(
    entry_ref, later_ref, forward_ref, backward_ref, decay_ref, tail_ref, leading_ref, step_ref,
    change_ref, raw_ref, rate_ref, x_ref, dy_ref, bin_ref, bout_ref, through_ref,
    entry_out, later_out, grad_x_out, grad_raw_out,
):
    _, groups, heads, length = tail_ref.shape
    row = lax.broadcasted_iota(jnp.int32, (length, length), 0)
    column = lax.broadcasted_iota(jnp.int32, (length, length), 1)
    from_here = (row >= column).astype(F32)
    before = 1.0 - from_here

    def by_head(v):
        return v.reshape(heads, v.shape[0] // heads, v.shape[1])

    def product(a, b):
        return lax.dot_general(a, b, (((1,), (1,)), ((), ())), preferred_element_type=F32)

    def summed(a, b):
        return lax.dot_general(
            a, b, (((1,), (0,)), ((), ())), precision=HIGH, preferred_element_type=F32
        )

    for b in range(CORES):
        for g in range(groups):
            entry, later = entry_ref[g], later_ref[g]
            if b == 1:
                carried_in = by_head(entry.astype(F32)) * decay_ref[0, g][:, :, None]
                entry = forward_ref[g] + carried_in.reshape(entry.shape)
                entry = entry.astype(BF16)
            else:
                carried_in = by_head(later.astype(F32)) * decay_ref[1, g][:, :, None]
                later = backward_ref[g] + carried_in.reshape(later.shape)
                later = later.astype(BF16)
            entry_out[b, g] = entry
            later_out[b, g] = later
            carried = by_head(product(later, bin_ref[b, g]))
            read = by_head(product(entry, bout_ref[b, g]))
            tail, step = tail_ref[b, g], step_ref[b, g]
            x = by_head(x_ref[b, g].astype(F32))
            dy = by_head(dy_ref[b, g].astype(F32))
            inner = by_head(through_ref[b, g]) + tail[:, None, :] * carried
            grad_x = step[:, None, :] * inner
            grad_x_out[b, g] = grad_x.reshape(x_ref.shape[2:]).astype(BF16)
            direct = jnp.sum(x * inner, axis=1)
            entry_term = leading_ref[b, g] * jnp.sum(read * dy, axis=1)
            exit_term = tail * step * jnp.sum(x * carried, axis=1)
            both = by_head(later.astype(F32) * entry.astype(F32))
            closing = decay_ref[b, g] * jnp.sum(jnp.sum(both, axis=1), axis=1, keepdims=True)
            grad_log = summed(change_ref[b, g] + entry_term, from_here) + summed(exit_term, before)
            grad_step = direct - rate_ref[g] * (grad_log + closing)
            grad_raw = grad_step * jax.nn.sigmoid(raw_ref[b, g])
            grad_raw_out[b, g] = grad_raw.astype(BF16)


def body(
    layer_input, dt_weight, dt_bias, decay_rate, ssm_input, in_basis, out_basis, out_cotangent
):
    upper = lax.axis_index("core") == 1

    def chosen(v, own):
        return jnp.where(upper == own, v[1], v[0])

    def in_order(own, other):
        return jnp.where(upper, jnp.stack([other, own]), jnp.stack([own, other]))

    tokens = layer_input[0]
    length, width = tokens.shape
    heads = dt_weight.shape[1] // CORES
    groups = in_basis.shape[2] // STATE // CORES
    per_group = heads // groups
    head_size = ssm_input.shape[2] // CORES // heads
    packs = LANES // heads
    rows = dt_weight.shape[0] // packs
    devices = lax.axis_size("fsdp")

    weight_half = chosen(jnp.stack(jnp.split(dt_weight, CORES, axis=1)), True)
    weight = copies_to(packed_rows(weight_half, packs), "fsdp").reshape(width // packs, LANES)
    both_tokens = jnp.stack([tokens, core_swap(tokens)]).reshape(CORES * length, width)

    sides = [v[0] for v in (ssm_input, out_cotangent, in_basis, out_basis)]
    cuts = [0]
    for side in sides:
        cuts.append(cuts[-1] + side.shape[1] // CORES)

    def picked(v, own):
        low, high = jnp.split(v, CORES, axis=1)
        return jnp.where(upper == own, high, low)

    other_sides = core_swap(jnp.concatenate([picked(side, False) for side in sides], axis=1))
    x_half, dy_half, bin_half, bout_half = (
        (picked(side, True), other_sides[:, cuts[i] : cuts[i + 1]])
        for i, side in enumerate(sides)
    )

    def tiled(pair):
        return in_order(*(jnp.stack(jnp.split(v, v.shape[1] // LANES, axis=1)) for v in pair))

    unit = jnp.eye(heads * head_size, dtype=BF16)

    def turned(pair):
        return jnp.einsum("bsc,cd->bds", in_order(*pair), unit, preferred_element_type=BF16)

    x_half, dy_half = turned(x_half), turned(dy_half)
    bin_half, bout_half = tiled(bin_half), tiled(bout_half)
    bias, rate = (
        chosen(v.reshape(CORES, heads, 1), True) for v in (dt_bias, decay_rate)
    )

    chunk = LANES * packs
    near = rows * packs
    target = jnp.arange(chunk)
    pack, place = target // LANES, target % LANES
    source = place // rows * near + pack * rows + place % rows
    order = (jnp.arange(chunk)[:, None] == source[None, :]).astype(BF16)
    columns = jnp.einsum(
        "pgc,cad->agdp",
        both_tokens.reshape(CORES * length, width // chunk, chunk),
        order.reshape(chunk, packs, LANES),
        preferred_element_type=BF16,
    ).reshape(packs, width // packs, CORES * length)

    product = jnp.einsum("akp,km->amp", columns, weight, preferred_element_type=F32)
    raw = bias + sum(product[a, a * heads : (a + 1) * heads] for a in range(packs))
    raw = in_order(raw[:, :length], raw[:, length:])
    step_size = jax.nn.softplus(raw)
    position = jnp.arange(length)
    lower = position[:, None] >= position[None, :]
    triangle = lower.astype(F32)
    cumulative = jnp.einsum("bhu,tu->bht", -rate * step_size, triangle, precision=HIGH)
    grid = (CORES, groups, per_group, length)
    cumulative = cumulative.reshape(grid)
    final = cumulative[..., -1:]
    step_grid = step_size.reshape(grid)
    tail = jnp.exp(final - cumulative)
    leading = jnp.exp(cumulative)
    block_decay = jnp.exp(final)
    x_half = x_half.reshape(CORES, groups, per_group, head_size, length)
    dy_half = dy_half.reshape(x_half.shape)
    bin_half = bin_half.reshape(CORES, groups, length, STATE)
    bout_half = bout_half.reshape(bin_half.shape)
    inputs = x_half.astype(F32)
    upstream = dy_half.astype(F32)
    tailed = ((tail * step_grid)[..., None, :] * inputs).astype(BF16)
    led = (leading[..., None, :] * upstream).astype(BF16)
    forward = jnp.einsum("bgkps,bgsn->bgkpn", tailed, bin_half, preferred_element_type=F32)
    backward = jnp.einsum("bgkpt,bgtn->bgkpn", led, bout_half, preferred_element_type=F32)
    factor = block_decay[..., None]
    chip_forward = forward[1] + factor[1] * forward[0]
    chip_backward = backward[0] + factor[0] * backward[1]

    spread = cumulative[..., :, None] - cumulative[..., None, :]
    decay_mat = jnp.where(lower, jnp.exp(jnp.where(lower, spread, 0.0)), 0.0)
    intersection = jnp.einsum("bgtn,bgsn->bgts", bout_half, bin_half, preferred_element_type=F32)
    weighted = (decay_mat * intersection[:, :, None]).astype(BF16)
    pair = jnp.einsum("bgkpt,bgkps->bgkts", dy_half, x_half, preferred_element_type=F32)
    through = jnp.einsum("bgkpt,bgkts->bgkps", dy_half, weighted, preferred_element_type=F32)
    scaled = decay_mat * pair * step_grid[..., None, :]
    joint = jnp.sum(scaled, axis=2).astype(BF16)
    moment = scaled * intersection[:, :, None]
    change = jnp.sum(moment, axis=-1) - jnp.sum(moment, axis=-2)
    local_b = jnp.einsum("bgts,bgtn->bgsn", joint, bout_half, preferred_element_type=F32)
    local_c = jnp.einsum("bgts,bgsn->bgtn", joint, bin_half, preferred_element_type=F32)
    local = [through, change, local_b, local_c]

    def together(got):
        got, *local[:] = lax.optimization_barrier((got, *local))
        return got

    flat = (heads, head_size, STATE)
    entry, later = carried_states(
        chip_forward.reshape(flat),
        chip_backward.reshape(flat),
        jnp.exp(final[0] + final[1]).reshape(heads),
        together,
    )
    through, change, local_b, local_c = local
    tall = (CORES, groups, per_group * head_size, LANES)
    entry, later, grad_x, grad_raw = pl.pallas_call(
        after_trade,
        out_shape=[jax.ShapeDtypeStruct(tall, BF16)] * 3 + [jax.ShapeDtypeStruct(grid, BF16)],
        cost_estimate=pl.CostEstimate(flops=2**29, bytes_accessed=2**23, transcendentals=2**13),
    )(
        entry.reshape(tall[1:]),
        later.reshape(tall[1:]),
        forward[0].reshape(tall[1:]),
        backward[1].reshape(tall[1:]),
        block_decay,
        tail,
        leading,
        step_grid,
        change,
        raw.reshape(grid),
        rate.reshape(groups, per_group, 1),
        x_half.reshape(tall),
        dy_half.reshape(tall),
        bin_half,
        bout_half,
        through.reshape(tall),
    )
    entry = entry.reshape(x_half.shape[:-1] + (STATE,))
    later = later.reshape(entry.shape)
    grad_raw = grad_raw.reshape(raw.shape)

    grad_raw = jnp.where(upper, grad_raw[::-1], grad_raw)
    grad_raw = jnp.concatenate([grad_raw[0], grad_raw[1]], axis=1)
    zero = jnp.zeros_like(grad_raw)
    placed = jnp.stack(
        [jnp.concatenate([grad_raw if i == a else zero for i in range(packs)]) for a in range(packs)]
    )
    partial = jnp.einsum("akp,amp->km", columns, placed, preferred_element_type=F32)
    tiles = partial.astype(BF16).reshape(devices, rows, LANES)
    tiles = lax.all_to_all(tiles, "fsdp", 0, 0, tiled=True)

    grad_b = jnp.einsum("bgkps,bgkpn->bgsn", tailed, later, preferred_element_type=F32)
    grad_b = (local_b + grad_b).astype(BF16)
    grad_c = jnp.einsum("bgkpt,bgkpn->bgtn", led, entry, preferred_element_type=F32)
    grad_c = (local_c + grad_c).astype(BF16)
    outs = jnp.concatenate(
        [v.reshape(CORES, -1, LANES) for v in (grad_x, grad_b, grad_c)], axis=1
    )
    own_outs = chosen(outs, True)
    other_outs = core_swap(chosen(outs, False))

    def joined(first, last):
        return in_order(own_outs[first:last], other_outs[first:last])

    size, basis = heads * head_size, groups * length
    out_x = joined(0, size).reshape(CORES * size, length).T
    outs_bc = []
    for first in (size, size + basis):
        whole = joined(first, first + basis).reshape(CORES * groups, length, STATE)
        outs_bc.append(jnp.concatenate([whole[g] for g in range(CORES * groups)], axis=1)[None])
    own_rows = jnp.sum(tiles.astype(F32), axis=0)
    blocks = copies_to(own_rows, SEQ).reshape(-1, CORES, rows, packs, heads)
    grad_weight = jnp.sum(blocks, axis=0).transpose(2, 1, 0, 3).reshape(dt_weight.shape)
    return (out_x[None], *outs_bc, grad_weight)


def solution(mesh):
    blocks = mesh.shape["seq"]
    split = Mesh(
        mesh.devices.reshape(mesh.shape["fsdp"], blocks // CORES, CORES), ("fsdp", *SEQ)
    )
    wide = P("fsdp", SEQ, None)
    return jax.shard_map(
        body,
        mesh=split,
        in_specs=(wide, P("fsdp", None), P(), P(), wide, wide, wide, wide),
        out_specs=(wide, wide, wide, P("fsdp", None)),
        check_vma=False,
    )
```
